32 devices in a mesh: dp: 2 (over x), tp: 16 (over y, z, core).
Axes of the slice: x: 2, y: 2, z: 4, core: 2. Of those that a mesh axis runs over, the one named last changes fastest.
Arguments:
- x: bfloat16 [128, 4608], P('dp'), parts along dimension 0
- k_cache: bfloat16 [128, 4096, 16, 128], P('dp', None, 'tp'), parts along dimension 0
- v_cache: bfloat16 [128, 4096, 16, 128], P('dp', None, 'tp'), parts along dimension 0
- gain_a: bfloat16 [4608], replicated
- wq: bfloat16 [4608, 4096], P(None, 'tp')
- wo: bfloat16 [4096, 4608], P('tp')
- gain_m: bfloat16 [4608], replicated
- w_gate: bfloat16 [4608, 36864], P(None, 'tp')
- w_up: bfloat16 [4608, 36864], P(None, 'tp')
- w_down: bfloat16 [36864, 4608], P('tp')
Outputs:
- output: bfloat16 [128, 4608], P('dp'), parts along dimension 0
There are 2 independent parts. The reference program is written for one: setup_inputs(seed, part) draws one part's arguments, and reference() takes and returns one part's arrays. A program takes and returns all parts, laid end to end along the dimension named above; an argument that names none is the same for every part.
All inputs are finite; a program needn't handle non-finite values.
Results may differ from the reference program's by a relative error of at most 0.017.
Values are sent between devices in bfloat16 or wider.
A program may use at most 2 GiB of HBM per device.

```python
import jax
import jax.numpy as jnp
from jax import lax

BATCH = 64
CACHE = 4096
D = 4608
HEADS = 32
KV_HEADS = 16
HEAD = 128
FF = 36864
THETA = 10000


def setup_inputs(seed: int = 0, part: int = 0) -> dict:
    kx, kc, kw, kn, kq, ko, km, kg, ku, kd = jax.random.split(jax.random.key(seed), 10)
    kx, kc, kw = (jax.random.fold_in(k, part) for k in (kx, kc, kw))

    def weights(key, rows, columns):
        return jax.random.normal(key, (rows, columns), jnp.float32) * rows**-0.5

    drawn = {
        "x": jax.random.normal(kx, (BATCH, D), jnp.float32),
        "k_cache": 2 * jax.random.normal(kc, (BATCH, CACHE, KV_HEADS, HEAD), jnp.float32),
        "v_cache": 4 * jax.random.normal(kw, (BATCH, CACHE, KV_HEADS, HEAD), jnp.float32),
        "gain_a": 1 + 0.1 * jax.random.normal(kn, (D,), jnp.float32),
        "wq": 2 * weights(kq, D, HEADS * HEAD),
        "wo": weights(ko, HEADS * HEAD, D),
        "gain_m": 1 + 0.1 * jax.random.normal(km, (D,), jnp.float32),
        "w_gate": weights(kg, D, FF),
        "w_up": weights(ku, D, FF),
        "w_down": 2 * weights(kd, FF, D),
    }
    return {k: v.astype(jnp.bfloat16) for k, v in drawn.items()}


def normed(x, gain):
    wide = x.astype(jnp.float32)
    scale = lax.rsqrt(jnp.mean(wide * wide, -1, keepdims=True) + 1e-6)
    return (wide * scale * gain.astype(jnp.float32)).astype(jnp.bfloat16)


def turned(t, place, theta):
    half = t.shape[-1] // 2
    angle = place.astype(jnp.float32)[:, None] * theta ** (-jnp.arange(half, dtype=jnp.float32) / half)
    cos, sin = jnp.cos(angle)[:, None], jnp.sin(angle)[:, None]
    a, b = t[..., :half].astype(jnp.float32), t[..., half:].astype(jnp.float32)
    return jnp.concatenate([a * cos - b * sin, b * cos + a * sin], -1).astype(jnp.bfloat16)


def matmul(a, w):
    return jnp.dot(a, w, preferred_element_type=jnp.float32).astype(jnp.bfloat16)


def einsum(form, a, b):
    return jnp.einsum(form, a.astype(jnp.float32), b.astype(jnp.float32))


def seen_by(a, wq, k_cache, v_cache, head, theta):
    batch, cache, kv_heads = k_cache.shape[:3]
    place = jnp.full((batch,), cache - 1)
    q = turned(matmul(a, wq).reshape(batch, -1, head), place, theta).reshape(batch, kv_heads, -1, head)
    scores = einsum("bgsd,bugd->bgsu", q, k_cache) * head**-0.5
    weights = jax.nn.softmax(scores, -1).astype(jnp.bfloat16)
    return einsum("bgsu,bugd->bgsd", weights, v_cache).astype(jnp.bfloat16).reshape(batch, -1)


def hidden_of(b, w_gate, w_up):
    gate = jnp.dot(b, w_gate, preferred_element_type=jnp.float32)
    up = jnp.dot(b, w_up, preferred_element_type=jnp.float32)
    return (jax.nn.silu(gate) * up).astype(jnp.bfloat16)


def reference(x, k_cache, v_cache, gain_a, wq, wo, gain_m, w_gate, w_up, w_down):
    seen = seen_by(normed(x, gain_a), wq, k_cache, v_cache, HEAD, THETA)
    h = (x.astype(jnp.float32) + jnp.dot(seen, wo, preferred_element_type=jnp.float32)).astype(jnp.bfloat16)
    hidden = hidden_of(normed(h, gain_m), w_gate, w_up)
    return (h.astype(jnp.float32) + jnp.dot(hidden, w_down, preferred_element_type=jnp.float32)).astype(jnp.bfloat16)
```

```python
import functools

import jax
import jax.numpy as jnp
from jax import lax
from jax.experimental import pallas as pl
from jax.experimental.pallas import tpu as pltpu
from jax.sharding import PartitionSpec as P

HEAD = 128
THETA = 10000
MESH = pl.DeviceIdType.MESH
F32, BF16 = jnp.float32, jnp.bfloat16


def normed(x, gain):
    wide = x.astype(jnp.float32)
    scale = lax.rsqrt(jnp.mean(wide * wide, -1, keepdims=True) + 1e-6)
    return (wide * scale * gain.astype(jnp.float32)).astype(jnp.bfloat16)


def turned(t, place, theta):
    half = t.shape[-1] // 2
    angle = place.astype(jnp.float32)[:, None] * theta ** (-jnp.arange(half, dtype=jnp.float32) / half)
    cos, sin = jnp.cos(angle)[:, None], jnp.sin(angle)[:, None]
    a, b = t[..., :half].astype(jnp.float32), t[..., half:].astype(jnp.float32)
    return jnp.concatenate([a * cos - b * sin, b * cos + a * sin], -1).astype(jnp.bfloat16)


def matmul(a, w):
    return jnp.dot(a, w, preferred_element_type=jnp.float32).astype(jnp.bfloat16)


def einsum(form, a, b):
    return jnp.einsum(form, a.astype(jnp.float32), b.astype(jnp.float32))


def seen_by(a, wq, k_cache, v_cache, head, theta):
    batch, cache, kv_heads = k_cache.shape[:3]
    place = jnp.full((batch,), cache - 1)
    q = turned(matmul(a, wq).reshape(batch, -1, head), place, theta).reshape(batch, kv_heads, -1, head)
    scores = einsum("bgsd,bugd->bgsu", q, k_cache) * head**-0.5
    weights = jax.nn.softmax(scores, -1).astype(jnp.bfloat16)
    return einsum("bgsu,bugd->bgsd", weights, v_cache).astype(jnp.bfloat16).reshape(batch, -1)


def hidden_of(b, w_gate, w_up):
    gate = jnp.dot(b, w_gate, preferred_element_type=jnp.float32)
    up = jnp.dot(b, w_up, preferred_element_type=jnp.float32)
    return (jax.nn.silu(gate) * up).astype(jnp.bfloat16)


def add_kernel(chips, t_ref, x_ref, o_ref, r0, s1, r1, a_send, a_recv, b_send, b_recv, c_send, c_recv, d_send, d_recv):
    wide = t_ref.shape[2] // 2
    me = lax.axis_index("tp")
    core, chip = me % 2, me // 2
    partner = me + 1 - 2 * core
    own = pl.ds(pl.multiple_of(core * wide, 128), wide)
    other = pl.ds(pl.multiple_of((1 - core) * wide, 128), wide)

    def to(o):
        return (chip + o) % chips

    def frm(o):
        return (chip + chips - o) % chips

    def remote(src, dst, send, recv, device):
        return pltpu.make_async_remote_copy(src_ref=src, dst_ref=dst, send_sem=send, recv_sem=recv, device_id={"tp": device}, device_id_type=MESH)

    barrier = pltpu.get_barrier_semaphore()
    pl.semaphore_signal(barrier, inc=1, device_id={"tp": partner}, device_id_type=MESH)
    for o in range(1, chips):
        pl.semaphore_signal(barrier, inc=1, device_id={"tp": to(o) * 2 + core}, device_id_type=MESH)
    pl.semaphore_wait(barrier, chips)

    halves = [remote(t_ref.at[to(o), :, other], r0.at[o], a_send.at[o], a_recv.at[o], partner) for o in range(chips)]
    order = list(range(1, chips)) + [0]
    for o in order:
        halves[o].start()
    terms = [None] + [remote(s1.at[o], r1.at[o], b_send.at[o], b_recv.at[o], to(o) * 2 + core) for o in range(1, chips)]
    for o in range(1, chips):
        halves[o].wait_recv()
        s1[o] = (t_ref[to(o), :, own].astype(F32) + r0[o].astype(F32)).astype(BF16)
        terms[o].start()
    halves[0].wait_recv()
    total = t_ref[chip, :, own].astype(F32) + r0[0].astype(F32)
    for o in range(1, chips):
        terms[o].wait_recv()
        total = total + r1[o].astype(F32)
    o_ref[chip, :, own] = (x_ref[chip, :, own].astype(F32) + total).astype(BF16)
    done = o_ref.at[chip, :, own]
    out = [None] + [remote(done, done, c_send.at[o], c_recv.at[o], to(o) * 2 + core) for o in range(1, chips)]
    over = [remote(done, done, d_send.at[0], d_recv.at[0], partner)]
    for o in range(1, chips):
        out[o].start()
    over[0].start()
    for o in range(1, chips):
        out[o].wait_recv()
        piece = o_ref.at[frm(o), :, own]
        over.append(remote(piece, piece, d_send.at[o], d_recv.at[o], partner))
        over[o].start()
    for o in range(chips):
        over[o].wait_recv()
    for o in range(chips):
        halves[o].wait_send()
        over[o].wait_send()
        if o:
            terms[o].wait_send()
            out[o].wait_send()


def added(x, term, cid):
    chips, d = 8, x.shape[1]
    blocks = (chips, x.shape[0] // chips, d)
    share = (chips, blocks[1], d // 2)
    sem = pltpu.SemaphoreType.DMA((chips,))
    out = pl.pallas_call(
        functools.partial(add_kernel, chips),
        out_shape=jax.ShapeDtypeStruct(blocks, BF16),
        in_specs=[pl.BlockSpec(memory_space=pltpu.VMEM)] * 2,
        out_specs=pl.BlockSpec(memory_space=pltpu.VMEM),
        scratch_shapes=[pltpu.VMEM(share, BF16)] * 3 + [sem] * 8,
        compiler_params=pltpu.CompilerParams(collective_id=cid, has_side_effects=True),
        name="added%d" % cid,
    )(term.astype(BF16).reshape(blocks), x.reshape(blocks))
    return out.reshape(x.shape)


def solution(mesh):
    def step(x, k_cache, v_cache, gain_a, wq, wo, gain_m, w_gate, w_up, w_down):
        seen = seen_by(normed(x, gain_a), wq, k_cache, v_cache, HEAD, THETA)
        h = added(x, jnp.dot(seen, wo, preferred_element_type=jnp.float32), 0)
        return added(h, jnp.dot(hidden_of(normed(h, gain_m), w_gate, w_up), w_down, preferred_element_type=jnp.float32), 1)

    states, cache, columns, rows_of = P("dp", None), P("dp", None, "tp", None), P(None, "tp"), P("tp", None)
    return jax.shard_map(
        step,
        mesh=mesh,
        in_specs=(states, cache, cache, P(None), columns, rows_of, P(None), columns, columns, rows_of),
        out_specs=states,
        check_vma=False,
    )
```

```python
import functools

import jax
import jax.numpy as jnp
import numpy as np
from jax import lax
from jax.experimental import pallas as pl
from jax.experimental.pallas import tpu as pltpu
from jax.sharding import PartitionSpec as P

HEAD = 128
THETA = 10000
CHIPS = 8
MESH = pl.DeviceIdType.MESH
F32, BF16 = jnp.float32, jnp.bfloat16
NT = (((1,), (1,)), ((), ()))


def rotation(place):
    half = HEAD // 2
    step = np.float32(THETA) ** (-np.arange(half, dtype=np.float32) / np.float32(half))
    angle = (np.float32(place) * step).astype(np.float64)
    cos, sin = np.cos(angle), np.sin(angle)
    return np.stack([np.concatenate([cos, cos]), np.concatenate([-sin, sin])]).astype(np.float32)


class Sum:
    def __init__(self, t, residual, out, place, wide, bufs, sems, half):
        self.t, self.residual, self.out, self.place, self.wide = t, residual, out, place, wide
        self.r0, self.s1, self.r1 = bufs
        self.sems = sems
        self.half = half
        me = lax.axis_index("tp")
        self.core, self.chip = me % 2, me // 2
        self.partner = me + 1 - 2 * self.core

    def to(self, o):
        return (self.chip + o) % CHIPS

    def at(self, j, core):
        block, column = self.place(j)
        return block, slice(None), pl.ds(pl.multiple_of(core * self.half + column, 128), self.wide)

    def remote(self, src, dst, kind, o, device):
        return pltpu.make_async_remote_copy(
            src_ref=src, dst_ref=dst, send_sem=self.sems.at[kind, o], recv_sem=self.sems.at[kind + 1, o],
            device_id={"tp": device}, device_id_type=MESH,
        )

    def halves(self, o):
        return self.remote(self.t.at[self.at(self.to(o), 1 - self.core)], self.r0.at[o], 0, o, self.partner)

    def terms(self, o):
        return self.remote(self.s1.at[o], self.r1.at[o], 2, o, self.to(o) * 2 + self.core)

    def shares(self, o):
        done = self.out.at[self.at(self.chip, self.core)]
        return self.remote(done, done, 4, o, self.to(o) * 2 + self.core)

    def over(self, o):
        piece = self.out.at[self.at((self.chip + CHIPS - o) % CHIPS, self.core)]
        return self.remote(piece, piece, 6, o, self.partner)

    def send_halves(self):
        for o in [*range(1, CHIPS), 0]:
            self.halves(o).start()

    def send_terms(self):
        for o in range(1, CHIPS):
            self.halves(o).wait_recv()
            self.s1[o] = (self.t[self.at(self.to(o), self.core)].astype(F32) + self.r0[o].astype(F32)).astype(BF16)
            self.terms(o).start()

    def finish(self):
        self.halves(0).wait_recv()
        mine = self.at(self.chip, self.core)
        total = self.t[mine].astype(F32) + self.r0[0].astype(F32)
        for o in range(1, CHIPS):
            self.terms(o).wait_recv()
            total = total + self.r1[o].astype(F32)
        self.out[mine] = (self.residual[mine].astype(F32) + total).astype(BF16)
        for o in range(1, CHIPS):
            self.shares(o).start()
        self.over(0).start()

    def forward(self):
        for o in range(1, CHIPS):
            self.shares(o).wait_recv()
            self.over(o).start()

    def settle(self):
        for o in range(CHIPS):
            self.over(o).wait_recv()
        for o in range(CHIPS):
            self.halves(o).wait_send()
            self.over(o).wait_send()
            if o:
                self.terms(o).wait_send()
                self.shares(o).wait_send()


def layer_kernel(
    turn_ref, x_hbm, k_hbm, v_hbm, ga_hbm, wq_hbm, wo_hbm, gm_hbm, wg_hbm, wu_hbm, wd_hbm, o_ref,
    ring, wo, x3, h3, t3, rows16, hidden, q_ref, seen, s_ref, ga, gm,
    r0a, s1a, r1a, r0b, s1b, r1b, r0c, s1c, r1c,
    ring_sem, misc_sem, sem_a, sem_b, sem_c,
):
    d = x3.shape[2]
    half = d // 2
    cache = k_hbm.shape[1]
    ff = wg_hbm.shape[1]
    groups = x3.shape[0]
    me = lax.axis_index("tp")
    core, chip = me % 2, me // 2
    partner = me + 1 - 2 * core

    barrier = pltpu.get_barrier_semaphore()
    pl.semaphore_signal(barrier, inc=1, device_id={"tp": partner}, device_id_type=MESH)
    for o in range(1, CHIPS):
        pl.semaphore_signal(barrier, inc=1, device_id={"tp": (chip + o) % CHIPS * 2 + core}, device_id_type=MESH)

    def copy(src, dst, sem):
        return pltpu.make_async_copy(src, dst, sem)

    def cache_copy(g, i, j):
        src = k_hbm if i < 4 else v_hbm
        b = g * 8 + 2 * (i % 4) + j
        return copy(src.at[b], ring.at[g % 3, i, 0:cache, j * HEAD:(j + 1) * HEAD], ring_sem.at[g % 3, i, j])

    def fill(g, slots=range(8)):
        for i in slots:
            for j in range(2):
                cache_copy(g, i, j).start()

    def ffn_slot(f):
        return (groups + f // 8) % 3, f % 8

    def up_copy(f):
        src = (wg_hbm, wu_hbm)[f % 2]
        at = ffn_slot(f)
        return copy(src.at[:, (f // 2) * 256:(f // 2 + 1) * 256], ring.at[at], ring_sem.at[at[0], at[1], 0])

    def down_column(k):
        side = 1 - core if k < 9 else core
        return pl.multiple_of(side * half + (k % 9) * 256, 128)

    def down_copy(k):
        at = ffn_slot(18 + k // 2)
        return copy(wd_hbm.at[:, pl.ds(down_column(k), 256)], ring.at[at[0], at[1], (k % 2) * ff:(k % 2 + 1) * ff], ring_sem.at[at[0], at[1], k % 2])

    def fill_ffn(slots):
        for f in slots:
            if f < 18:
                up_copy(f).start()
            else:
                down_copy(2 * (f - 18)).start()
                down_copy(2 * (f - 18) + 1).start()

    x_copy = copy(x_hbm, x3, misc_sem.at[0])
    ga_copy = copy(ga_hbm, ga, misc_sem.at[1])
    wq_copy = copy(wq_hbm, ring.at[2, 7], ring_sem.at[2, 7, 0])
    wo_copy = copy(wo_hbm, wo, misc_sem.at[2])
    gm_copy = copy(gm_hbm, gm, misc_sem.at[3])
    x_copy.start()
    ga_copy.start()
    wq_copy.start()
    fill(0)
    fill(1)
    fill(2, range(7))
    wo_copy.start()
    gm_copy.start()

    def norm(src, gain):
        def pair(i, carry):
            wide = jnp.concatenate([src[2 * i], src[2 * i + 1]], axis=0).astype(F32)
            scale = lax.rsqrt(jnp.mean(wide * wide, -1, keepdims=True) + 1e-6)
            rows16[pl.ds(pl.multiple_of(16 * i, 16), 16), :] = (wide * scale * gain[...].astype(F32)).astype(BF16)
            return carry
        lax.fori_loop(0, groups // 2, pair, 0)

    x_copy.wait()
    ga_copy.wait()
    norm(x3, ga)
    wq_copy.wait()
    q = jnp.dot(rows16[...], ring[2, 7], preferred_element_type=F32).astype(BF16).astype(F32)
    fill(2, [7])
    turned = []
    for s in range(2):
        t = q[:, s * HEAD:(s + 1) * HEAD]
        turned.append(t * turn_ref[0:1, :] + pltpu.roll(t, HEAD // 2, 1) * turn_ref[1:2, :])
    for g in range(groups):
        q_ref[g] = jnp.concatenate([t[8 * g:8 * g + 8] for t in turned], axis=0).astype(BF16).astype(F32)
    wo_copy.wait()
    pl.semaphore_wait(barrier, CHIPS)

    def chunk_place(first):
        return lambda j: (first + j // 2, (j % 2) * (half // 2))

    sum_a = Sum(t3, x3, h3, chunk_place(0), half // 2, (r0a, s1a, r1a), sem_a, half)
    sum_b = Sum(t3, x3, h3, chunk_place(groups // 2), half // 2, (r0b, s1b, r1b), sem_b, half)
    sum_c = Sum(t3, h3, o_ref, lambda j: (j, 0), half, (r0c, s1c, r1c), sem_c, half)

    def attend(g):
        row = lax.broadcasted_iota(jnp.int32, (16, HEAD), 0) % 8
        base = g % 3
        q16 = q_ref[g]
        for i in range(4):
            for j in range(2):
                cache_copy(g, i, j).wait()
        lhs = [
            jnp.concatenate([jnp.where(row == 2 * p + j, q16, 0.0) for j in range(2)], axis=1).astype(BF16)
            for p in range(4)
        ]
        chunk = 512
        for c in range(0, cache, chunk):
            s = None
            for p in range(4):
                part = lax.dot_general(lhs[p], ring[base, p, c:c + chunk, :], NT, preferred_element_type=F32)
                s = part if s is None else s + part
            s_ref[:, c:c + chunk] = s
        s = s_ref[...] * HEAD**-0.5
        e = jnp.exp(s - jnp.max(s, -1, keepdims=True))
        w = (e * (1.0 / jnp.sum(e, -1, keepdims=True))).astype(BF16)
        for i in range(4, 8):
            for j in range(2):
                cache_copy(g, i, j).wait()
        acc = jnp.zeros((16, HEAD), F32)
        for p in range(4):
            got = jnp.dot(w, ring[base, 4 + p, 0:cache, :], preferred_element_type=F32)
            for j in range(2):
                acc = jnp.where(row == 2 * p + j, got[:, j * HEAD:(j + 1) * HEAD], acc)
        at = pl.ds(pl.multiple_of(8 * g, 8), 8)
        seen[at, 0:HEAD] = acc[0:8]
        seen[at, HEAD:] = acc[8:16]

    def project(first):
        count = groups // 2
        rows = seen[8 * first:8 * (first + count), :].astype(BF16)
        for c in range(0, d, 768):
            term = jnp.dot(rows, wo[:, c:c + 768], preferred_element_type=F32)
            for i in range(count):
                t3[first + i, :, c:c + 768] = term[8 * i:8 * i + 8].astype(BF16)

    def body(g, carry):
        attend(g)
        @pl.when(g < groups - 3)
        def _():
            fill(g + 3)
        for n in range(3):
            @pl.when(g == groups - 3 + n)
            def _():
                fill_ffn(range(8 * n, 8 * n + 8))
        @pl.when(g == groups // 2 - 1)
        def _():
            project(0)
            sum_a.send_halves()
        @pl.when(g == groups // 2)
        def _():
            sum_a.send_terms()
        @pl.when(g == groups // 2 + 1)
        def _():
            sum_a.finish()
        @pl.when(g == groups // 2 + 2)
        def _():
            sum_a.forward()
        return carry

    lax.fori_loop(0, groups, body, 0)
    project(groups // 2)
    sum_b.send_halves()
    sum_b.send_terms()
    sum_a.settle()
    sum_b.finish()
    sum_b.forward()
    gm_copy.wait()
    sum_b.settle()
    norm(h3, gm)

    for i in range(3):
        for f in range(6 * i, 6 * i + 6):
            up_copy(f).wait()
        for n in range(3 * i, 3 * i + 3):
            gate = jnp.dot(rows16[...], ring[ffn_slot(2 * n)], preferred_element_type=F32)
            up = jnp.dot(rows16[...], ring[ffn_slot(2 * n + 1)], preferred_element_type=F32)
            hidden[:, n * 256:(n + 1) * 256] = (jax.nn.silu(gate) * up).astype(BF16)
        if i == 0:
            fill_ffn(range(24, 27))

    def down(blocks):
        for k in blocks:
            down_copy(k).wait()
        for k in blocks:
            at = ffn_slot(18 + k // 2)
            term = jnp.dot(hidden[...], ring[at[0], at[1], (k % 2) * ff:(k % 2 + 1) * ff, :], preferred_element_type=F32)
            for i in range(groups):
                t3[i, :, pl.ds(down_column(k), 256)] = term[8 * i:8 * i + 8].astype(BF16)

    down(range(0, 9))
    sum_c.send_halves()
    down(range(9, 18))
    sum_c.send_terms()
    sum_c.finish()
    sum_c.forward()
    sum_c.settle()


def layer(x, k_cache, v_cache, gain_a, wq, wo, gain_m, w_gate, w_up, w_down):
    rows, d = x.shape
    cache = k_cache.shape[1]
    ff = w_gate.shape[1]
    blocks = (CHIPS, rows // CHIPS, d)
    wide = d // 4
    small, large = (CHIPS, 8, wide), (CHIPS, 8, 2 * wide)
    dma = pltpu.SemaphoreType.DMA
    anywhere = pl.BlockSpec(memory_space=pl.ANY)
    vmem = pl.BlockSpec(memory_space=pltpu.VMEM)
    scratch = [
        pltpu.VMEM((3, 8, d, 256), BF16),
        pltpu.VMEM(wo.shape, BF16),
        pltpu.VMEM(blocks, BF16),
        pltpu.VMEM(blocks, BF16),
        pltpu.VMEM(blocks, BF16),
        pltpu.VMEM((rows, d), BF16),
        pltpu.VMEM((rows, ff), BF16),
        pltpu.VMEM((rows // 8, 16, HEAD), F32),
        pltpu.VMEM((rows, 2 * HEAD), F32),
        pltpu.VMEM((16, cache), F32),
        pltpu.VMEM((1, d), BF16),
        pltpu.VMEM((1, d), BF16),
    ]
    scratch += [pltpu.VMEM(small, BF16)] * 6 + [pltpu.VMEM(large, BF16)] * 3
    scratch += [dma((3, 8, 2)), dma((4,))] + [dma((8, CHIPS))] * 3
    out = pl.pallas_call(
        layer_kernel,
        out_shape=jax.ShapeDtypeStruct(blocks, BF16),
        in_specs=[vmem] + [anywhere] * 10,
        out_specs=vmem,
        scratch_shapes=scratch,
        compiler_params=pltpu.CompilerParams(collective_id=0, has_side_effects=True, vmem_limit_bytes=66_200_000),
        name="layer",
    )(
        jnp.asarray(rotation(cache - 1)), x.reshape(blocks), k_cache.reshape(rows, cache, HEAD), v_cache.reshape(rows, cache, HEAD),
        gain_a.reshape(1, d), wq, wo, gain_m.reshape(1, d), w_gate, w_up, w_down,
    )
    return out.reshape(x.shape)


def solution(mesh):
    states, cache, columns, rows_of = P("dp", None), P("dp", None, "tp", None), P(None, "tp"), P("tp", None)
    return jax.shard_map(
        layer,
        mesh=mesh,
        in_specs=(states, cache, cache, P(None), columns, rows_of, P(None), columns, columns, rows_of),
        out_specs=states,
        check_vma=False,
    )
```

```python
import functools

import jax
import jax.numpy as jnp
import numpy as np
from jax import lax
from jax.experimental import pallas as pl
from jax.experimental.pallas import tpu as pltpu
from jax.sharding import PartitionSpec as P

HEAD = 128
THETA = 10000
CHIPS = 8
PARTS = 3
KEYS, VALUES = range(4), range(4, 8)
MESH = pl.DeviceIdType.MESH
F32, BF16 = jnp.float32, jnp.bfloat16
NT = (((1,), (1,)), ((), ()))


def rotation(place):
    half = HEAD // 2
    step = np.float32(THETA) ** (-np.arange(half, dtype=np.float32) / np.float32(half))
    angle = (np.float32(place) * step).astype(np.float64)
    cos, sin = np.cos(angle), np.sin(angle)
    return np.stack([np.concatenate([cos, cos]), np.concatenate([-sin, sin])]).astype(np.float32)


class Sum:
    def __init__(self, t, residual, out, place, wide, bufs, sems, half):
        self.t, self.residual, self.out, self.place, self.wide = t, residual, out, place, wide
        self.r0, self.s1, self.r1 = bufs
        self.sems = sems
        self.half = half
        me = lax.axis_index("tp")
        self.core, self.chip = me % 2, me // 2
        self.partner = me + 1 - 2 * self.core

    def to(self, o):
        return (self.chip + o) % CHIPS

    def at(self, j, core):
        block, column = self.place(j)
        return block, slice(None), pl.ds(pl.multiple_of(core * self.half + column, 128), self.wide)

    def remote(self, src, dst, kind, o, device):
        return pltpu.make_async_remote_copy(
            src_ref=src, dst_ref=dst, send_sem=self.sems.at[kind, o], recv_sem=self.sems.at[kind + 1, o],
            device_id={"tp": device}, device_id_type=MESH,
        )

    def halves(self, o):
        return self.remote(self.t.at[self.at(self.to(o), 1 - self.core)], self.r0.at[o], 0, o, self.partner)

    def terms(self, o):
        return self.remote(self.s1.at[o], self.r1.at[o], 2, o, self.to(o) * 2 + self.core)

    def shares(self, o):
        done = self.out.at[self.at(self.chip, self.core)]
        return self.remote(done, done, 4, o, self.to(o) * 2 + self.core)

    def over(self, o):
        piece = self.out.at[self.at((self.chip + CHIPS - o) % CHIPS, self.core)]
        return self.remote(piece, piece, 6, o, self.partner)

    def send_halves(self):
        for o in [*range(1, CHIPS), 0]:
            self.halves(o).start()

    def send_terms(self):
        for o in range(1, CHIPS):
            self.halves(o).wait_recv()
            self.s1[o] = (self.t[self.at(self.to(o), self.core)].astype(F32) + self.r0[o].astype(F32)).astype(BF16)
            self.terms(o).start()

    def finish(self):
        self.halves(0).wait_recv()
        mine = self.at(self.chip, self.core)
        total = self.t[mine].astype(F32) + self.r0[0].astype(F32)
        for o in range(1, CHIPS):
            self.terms(o).wait_recv()
            total = total + self.r1[o].astype(F32)
        self.out[mine] = (self.residual[mine].astype(F32) + total).astype(BF16)
        for o in range(1, CHIPS):
            self.shares(o).start()
        self.over(0).start()

    def forward(self):
        for o in range(1, CHIPS):
            self.shares(o).wait_recv()
            self.over(o).start()

    def settle(self):
        for o in range(CHIPS):
            self.over(o).wait_recv()
        for o in range(CHIPS):
            self.halves(o).wait_send()
            self.over(o).wait_send()
            if o:
                self.terms(o).wait_send()
                self.shares(o).wait_send()


def layer_kernel(
    turn_ref, x_hbm, k_hbm, v_hbm, ga_hbm, wq_hbm, wo_hbm, gm_hbm, wg_hbm, wu_hbm, wd_hbm, o_ref,
    ring, wo, x3, h3, t3, rows16, hidden, q_ref, seen, s_ref, ga, gm,
    r0a, s1a, r1a, r0b, s1b, r1b, r0c, s1c, r1c,
    ring_sem, misc_sem, sem_a, sem_b, sem_c,
):
    d = x3.shape[2]
    half = d // 2
    cache = k_hbm.shape[1]
    ff = wg_hbm.shape[1]
    groups = x3.shape[0]
    me = lax.axis_index("tp")
    core, chip = me % 2, me // 2
    partner = me + 1 - 2 * core

    barrier = pltpu.get_barrier_semaphore()
    pl.semaphore_signal(barrier, inc=1, device_id={"tp": partner}, device_id_type=MESH)
    for o in range(1, CHIPS):
        pl.semaphore_signal(barrier, inc=1, device_id={"tp": (chip + o) % CHIPS * 2 + core}, device_id_type=MESH)

    def copy(src, dst, sem):
        return pltpu.make_async_copy(src, dst, sem)

    def cache_copy(g, i, j):
        src = k_hbm if i < 4 else v_hbm
        b = g * 8 + 2 * (i % 4) + j
        return copy(src.at[b], ring.at[g % 3, i, 0:cache, j * HEAD:(j + 1) * HEAD], ring_sem.at[g % 3, i, j])

    def fill(g, slots=range(8)):
        for i in slots:
            for j in range(2):
                cache_copy(g, i, j).start()

    def ffn_slot(f):
        return (groups + f // 8) % 3, f % 8

    def up_copy(f):
        src = (wg_hbm, wu_hbm)[f % 2]
        at = ffn_slot(f)
        return copy(src.at[:, (f // 2) * 256:(f // 2 + 1) * 256], ring.at[at], ring_sem.at[at[0], at[1], 0])

    def down_column(k):
        side = core if k % 6 >= 3 else 1 - core
        return pl.multiple_of(side * half + k // 6 * (half // PARTS) + k % 3 * 256, 128)

    def down_copy(k):
        at = ffn_slot(18 + k // 2)
        return copy(wd_hbm.at[:, pl.ds(down_column(k), 256)], ring.at[at[0], at[1], (k % 2) * ff:(k % 2 + 1) * ff], ring_sem.at[at[0], at[1], k % 2])

    def fill_ffn(slots):
        for f in slots:
            if f < 18:
                up_copy(f).start()
            else:
                down_copy(2 * (f - 18)).start()
                down_copy(2 * (f - 18) + 1).start()

    x_copy = copy(x_hbm, x3, misc_sem.at[0])
    ga_copy = copy(ga_hbm, ga, misc_sem.at[1])
    wq_copy = copy(wq_hbm, ring.at[2, 7], ring_sem.at[2, 7, 0])
    wo_copy = copy(wo_hbm, wo, misc_sem.at[2])
    gm_copy = copy(gm_hbm, gm, misc_sem.at[3])
    x_copy.start()
    ga_copy.start()
    wq_copy.start()
    fill(0, KEYS)

    def norm(src, gain):
        def pair(i, carry):
            wide = jnp.concatenate([src[2 * i], src[2 * i + 1]], axis=0).astype(F32)
            scale = lax.rsqrt(jnp.mean(wide * wide, -1, keepdims=True) + 1e-6)
            rows16[pl.ds(pl.multiple_of(16 * i, 16), 16), :] = (wide * scale * gain[...].astype(F32)[None, :]).astype(BF16)
            return carry
        lax.fori_loop(0, groups // 2, pair, 0)

    x_copy.wait()
    ga_copy.wait()
    norm(x3, ga)
    fill(0, VALUES)
    wo_copy.start()
    gm_copy.start()
    wq_copy.wait()
    q = jnp.dot(rows16[...], ring[2, 7], preferred_element_type=F32).astype(BF16).astype(F32)
    turned = []
    for s in range(2):
        t = q[:, s * HEAD:(s + 1) * HEAD]
        turned.append(t * turn_ref[0:1, :] + pltpu.roll(t, HEAD // 2, 1) * turn_ref[1:2, :])
    for g in range(groups):
        q_ref[g] = jnp.concatenate([t[8 * g:8 * g + 8] for t in turned], axis=0).astype(BF16).astype(F32)
    wo_copy.wait()
    pl.semaphore_wait(barrier, CHIPS)

    def chunk_place(first, column):
        return lambda j: (first + j // 2, (j % 2) * (half // 2) + column)

    def bufs(*args):
        return [buf.at[args[-1]] for buf in args[:-1]]

    sum_a = Sum(t3, x3, h3, chunk_place(0, 0), half // 2, bufs(r0a, s1a, r1a, 0), sem_a.at[0], half)
    sums_b = [
        Sum(t3, x3, h3, chunk_place(groups // 2, n * (half // 2 // PARTS)), half // 2 // PARTS, bufs(r0b, s1b, r1b, n), sem_b.at[n], half)
        for n in range(PARTS)
    ]
    sums_c = [
        Sum(t3, h3, o_ref, lambda j, n=n: (j, n * (half // PARTS)), half // PARTS, bufs(r0c, s1c, r1c, n), sem_c.at[n], half) for n in range(PARTS)
    ]

    def attend(g):
        row = lax.broadcasted_iota(jnp.int32, (16, HEAD), 0) % 8
        base = g % 3
        q16 = q_ref[g]
        for i in range(4):
            for j in range(2):
                cache_copy(g, i, j).wait()
        @pl.when(g < groups - 1)
        def _():
            fill(g + 1, KEYS)
        lhs = [
            jnp.concatenate([jnp.where(row == 2 * p + j, q16, 0.0) for j in range(2)], axis=1).astype(BF16)
            for p in range(4)
        ]
        chunk = 512
        for c in range(0, cache, chunk):
            s = None
            for p in range(4):
                part = lax.dot_general(lhs[p], ring[base, p, c:c + chunk, :], NT, preferred_element_type=F32)
                s = part if s is None else s + part
            s_ref[:, c:c + chunk] = s
        s = s_ref[...] * HEAD**-0.5
        e = jnp.exp(s - jnp.max(s, -1, keepdims=True))
        w = (e * (1.0 / jnp.sum(e, -1, keepdims=True))).astype(BF16)
        for i in range(4, 8):
            for j in range(2):
                cache_copy(g, i, j).wait()
        @pl.when(g < groups - 1)
        def _():
            fill(g + 1, VALUES)
        @pl.when(g == groups - 1)
        def _():
            fill_ffn(range(8))
        acc = jnp.zeros((16, HEAD), F32)
        for p in range(4):
            got = jnp.dot(w, ring[base, 4 + p, 0:cache, :], preferred_element_type=F32)
            for j in range(2):
                acc = jnp.where(row == 2 * p + j, got[:, j * HEAD:(j + 1) * HEAD], acc)
        at = pl.ds(pl.multiple_of(8 * g, 8), 8)
        seen[at, 0:HEAD] = acc[0:8]
        seen[at, HEAD:] = acc[8:16]

    def project(first):
        count = groups // 2
        rows = seen[8 * first:8 * (first + count), :].astype(BF16)
        for c in range(0, d, 768):
            term = jnp.dot(rows, wo[:, c:c + 768], preferred_element_type=F32)
            for i in range(count):
                t3[first + i, :, c:c + 768] = term[8 * i:8 * i + 8].astype(BF16)

    def body(g, carry):
        attend(g)
        @pl.when(g == groups // 2 - 1)
        def _():
            project(0)
            sum_a.send_halves()
        @pl.when(g == groups // 2)
        def _():
            sum_a.send_terms()
        @pl.when(g == groups // 2 + 1)
        def _():
            sum_a.finish()
        @pl.when(g == groups // 2 + 2)
        def _():
            sum_a.forward()
        return carry

    lax.fori_loop(0, groups, body, 0)
    project(groups // 2)
    for b in sums_b:
        b.send_halves()
    for b in sums_b:
        b.send_terms()
    fill_ffn(range(8, 12))
    sum_a.settle()
    for b in sums_b:
        b.finish()
    fill_ffn(range(12, 20))
    for b in sums_b:
        b.forward()
    gm_copy.wait()
    for b in sums_b:
        b.settle()
    fill_ffn(range(20, 24))
    norm(h3, gm)

    for i in range(3):
        for f in range(6 * i, 6 * i + 6):
            up_copy(f).wait()
        for n in range(3 * i, 3 * i + 3):
            gate = jnp.dot(rows16[...], ring[ffn_slot(2 * n)], preferred_element_type=F32)
            up = jnp.dot(rows16[...], ring[ffn_slot(2 * n + 1)], preferred_element_type=F32)
            hidden[:, n * 256:(n + 1) * 256] = (jax.nn.silu(gate) * up).astype(BF16)
        if i == 0:
            fill_ffn(range(24, 27))

    def down(blocks):
        for k in blocks:
            down_copy(k).wait()
        for k in blocks:
            at = ffn_slot(18 + k // 2)
            term = jnp.dot(hidden[...], ring[at[0], at[1], (k % 2) * ff:(k % 2 + 1) * ff, :], preferred_element_type=F32)
            for i in range(groups):
                t3[i, :, pl.ds(down_column(k), 256)] = term[8 * i:8 * i + 8].astype(BF16)

    c0, c1, c2 = sums_c
    down(range(0, 3))
    c0.send_halves()
    down(range(3, 6))
    down(range(6, 9))
    c1.send_halves()
    c0.send_terms()
    down(range(9, 12))
    down(range(12, 15))
    c2.send_halves()
    c1.send_terms()
    down(range(15, 18))
    c2.send_terms()
    c0.finish()
    c1.finish()
    c0.forward()
    c2.finish()
    c1.forward()
    c2.forward()
    for c in sums_c:
        c.settle()


def layer(x, k_cache, v_cache, gain_a, wq, wo, gain_m, w_gate, w_up, w_down):
    rows, d = x.shape
    cache = k_cache.shape[1]
    ff = w_gate.shape[1]
    blocks = (CHIPS, rows // CHIPS, d)
    wide = d // 4
    whole, small, large = (1, CHIPS, 8, wide), (PARTS, CHIPS, 8, wide // PARTS), (PARTS, CHIPS, 8, 2 * wide // PARTS)
    dma = pltpu.SemaphoreType.DMA
    anywhere = pl.BlockSpec(memory_space=pl.ANY)
    vmem = pl.BlockSpec(memory_space=pltpu.VMEM)
    scratch = [
        pltpu.VMEM((3, 8, d, 256), BF16),
        pltpu.VMEM(wo.shape, BF16),
        pltpu.VMEM(blocks, BF16),
        pltpu.VMEM(blocks, BF16),
        pltpu.VMEM(blocks, BF16),
        pltpu.VMEM((rows, d), BF16),
        pltpu.VMEM((rows, ff), BF16),
        pltpu.VMEM((rows // 8, 16, HEAD), F32),
        pltpu.VMEM((rows, 2 * HEAD), F32),
        pltpu.VMEM((16, cache), F32),
        pltpu.VMEM((d,), BF16),
        pltpu.VMEM((d,), BF16),
    ]
    scratch += [pltpu.VMEM(whole, BF16)] * 3 + [pltpu.VMEM(small, BF16)] * 3 + [pltpu.VMEM(large, BF16)] * 3
    scratch += [dma((3, 8, 2)), dma((4,))] + [dma((1, 8, CHIPS))] + [dma((PARTS, 8, CHIPS))] * 2
    out = pl.pallas_call(
        layer_kernel,
        out_shape=jax.ShapeDtypeStruct(blocks, BF16),
        in_specs=[vmem] + [anywhere] * 10,
        out_specs=vmem,
        scratch_shapes=scratch,
        compiler_params=pltpu.CompilerParams(collective_id=0, has_side_effects=True, vmem_limit_bytes=66_200_000),
        name="layer",
    )(
        jnp.asarray(rotation(cache - 1)), x.reshape(blocks), k_cache.reshape(rows, cache, HEAD), v_cache.reshape(rows, cache, HEAD),
        gain_a, wq, wo, gain_m, w_gate, w_up, w_down,
    )
    return out.reshape(x.shape)


def solution(mesh):
    states, cache, columns, rows_of = P("dp", None), P("dp", None, "tp", None), P(None, "tp"), P("tp", None)
    return jax.shard_map(
        layer,
        mesh=mesh,
        in_specs=(states, cache, cache, P(None), columns, rows_of, P(None), columns, columns, rows_of),
        out_specs=states,
        check_vma=False,
    )
```

```python
import functools

import jax
import jax.numpy as jnp
import numpy as np
from jax import lax
from jax.experimental import pallas as pl
from jax.experimental.pallas import tpu as pltpu
from jax.sharding import PartitionSpec as P

HEAD = 128
THETA = 10000
CHIPS = 8
PARTS = 3
KEYS, VALUES = range(4), range(4, 8)
MESH = pl.DeviceIdType.MESH
F32, BF16 = jnp.float32, jnp.bfloat16
NT = (((1,), (1,)), ((), ()))


def rotation(place):
    half = HEAD // 2
    step = np.float32(THETA) ** (-np.arange(half, dtype=np.float32) / np.float32(half))
    angle = (np.float32(place) * step).astype(np.float64)
    cos, sin = np.cos(angle), np.sin(angle)
    return np.stack([np.concatenate([cos, cos]), np.concatenate([-sin, sin])]).astype(np.float32)


class Sum:
    def __init__(self, t, residual, out, place, wide, bufs, sems, owners=CHIPS):
        self.t, self.residual, self.out, self.place, self.wide, self.owners = t, residual, out, place, wide, owners
        self.r0, self.s1, self.r1 = bufs
        self.sems = sems
        me = lax.axis_index("tp")
        self.core, self.chip = me % 2, me // 2
        self.partner = me + 1 - 2 * self.core

    def to(self, o):
        return (self.chip + o) % CHIPS

    def frm(self, o):
        return (self.chip + CHIPS - o) % CHIPS

    def at(self, j, core):
        block, column = self.place(j, core)
        return block, slice(None), pl.ds(pl.multiple_of(column, 128), self.wide)

    def owned(self, j, act):
        if self.owners == CHIPS:
            act()
        else:
            pl.when(j < self.owners)(act)

    def remote(self, src, dst, kind, o, device):
        return pltpu.make_async_remote_copy(
            src_ref=src, dst_ref=dst, send_sem=self.sems.at[kind, o], recv_sem=self.sems.at[kind + 1, o],
            device_id={"tp": device}, device_id_type=MESH,
        )

    def halves(self, o):
        return self.remote(self.t.at[self.at(self.to(o), 1 - self.core)], self.r0.at[o], 0, o, self.partner)

    def terms(self, o):
        return self.remote(self.s1.at[o], self.r1.at[o], 2, o, self.to(o) * 2 + self.core)

    def shares(self, o, chip):
        done = self.out.at[self.at(chip, self.core)]
        return self.remote(done, done, 4, o, self.to(o) * 2 + self.core)

    def over(self, o):
        piece = self.out.at[self.at(self.frm(o), self.core)]
        return self.remote(piece, piece, 6, o, self.partner)

    def send_halves(self):
        for o in [*range(1, CHIPS), 0]:
            self.owned(self.to(o), lambda o=o: self.halves(o).start())

    def send_terms(self):
        def send(o):
            self.halves(o).wait_recv()
            self.s1[o] = (self.t[self.at(self.to(o), self.core)].astype(F32) + self.r0[o].astype(F32)).astype(BF16)
            self.terms(o).start()

        for o in range(1, CHIPS):
            self.owned(self.to(o), lambda o=o: send(o))

    def finish(self):
        def act():
            self.halves(0).wait_recv()
            mine = self.at(self.chip, self.core)
            total = self.t[mine].astype(F32) + self.r0[0].astype(F32)
            for o in range(1, CHIPS):
                self.terms(o).wait_recv()
                total = total + self.r1[o].astype(F32)
            self.out[mine] = (self.residual[mine].astype(F32) + total).astype(BF16)
            for o in range(1, CHIPS):
                self.shares(o, self.chip).start()
            self.over(0).start()

        self.owned(self.chip, act)

    def forward(self):
        def act(o):
            self.shares(o, self.frm(o)).wait_recv()
            self.over(o).start()

        for o in range(1, CHIPS):
            self.owned(self.frm(o), lambda o=o: act(o))

    def settle(self):
        for o in range(CHIPS):
            self.owned(self.frm(o), lambda o=o: self.over(o).wait_recv())

    def sent(self):
        for o in range(CHIPS):
            self.owned(self.to(o), lambda o=o: self.halves(o).wait_send())
            self.owned(self.frm(o), lambda o=o: self.over(o).wait_send())
            if o:
                self.owned(self.to(o), lambda o=o: self.terms(o).wait_send())
                self.owned(self.chip, lambda o=o: self.shares(o, self.chip).wait_send())


def layer_kernel(
    turn_ref, x_hbm, k_hbm, v_hbm, ga_hbm, wq_hbm, wo_hbm, gm_hbm, wg_hbm, wu_hbm, wd_hbm, o_ref,
    ring, wo, x3, h3, t3, rows16, hidden, q_ref, seen, s_ref, ga, gm,
    r0a, s1a, r1a, r0b, s1b, r1b, r0c, s1c, r1c,
    ring_sem, misc_sem, sem_a, sem_b, sem_c,
):
    d = x3.shape[2]
    half = d // 2
    cache = k_hbm.shape[1]
    ff = wg_hbm.shape[1]
    groups = x3.shape[0]
    me = lax.axis_index("tp")
    core, chip = me % 2, me // 2
    partner = me + 1 - 2 * core

    barrier = pltpu.get_barrier_semaphore()
    pl.semaphore_signal(barrier, inc=1, device_id={"tp": partner}, device_id_type=MESH)
    for o in range(1, CHIPS):
        pl.semaphore_signal(barrier, inc=1, device_id={"tp": (chip + o) % CHIPS * 2 + core}, device_id_type=MESH)

    def copy(src, dst, sem):
        return pltpu.make_async_copy(src, dst, sem)

    def cache_copy(g, i, j):
        src = k_hbm if i < 4 else v_hbm
        b = g * 8 + 2 * (i % 4) + j
        return copy(src.at[b], ring.at[g % 3, i, 0:cache, j * HEAD:(j + 1) * HEAD], ring_sem.at[g % 3, i, j])

    def fill(g, slots=range(8)):
        for i in slots:
            for j in range(2):
                cache_copy(g, i, j).start()

    def ffn_slot(f):
        return (groups + f // 8) % 3, f % 8

    def up_copy(f):
        src = (wg_hbm, wu_hbm)[f % 2]
        at = ffn_slot(f)
        return copy(src.at[:, (f // 2) * 256:(f // 2 + 1) * 256], ring.at[at], ring_sem.at[at[0], at[1], 0])

    def down_column(k):
        side = core if k % 6 >= 3 else 1 - core
        return pl.multiple_of(side * half + k // 6 * (half // PARTS) + k % 3 * 256, 128)

    def down_copy(k):
        at = ffn_slot(18 + k // 2)
        return copy(wd_hbm.at[:, pl.ds(down_column(k), 256)], ring.at[at[0], at[1], (k % 2) * ff:(k % 2 + 1) * ff], ring_sem.at[at[0], at[1], k % 2])

    def fill_ffn(slots):
        for f in slots:
            if f < 18:
                up_copy(f).start()
            else:
                down_copy(2 * (f - 18)).start()
                down_copy(2 * (f - 18) + 1).start()

    x_copy = copy(x_hbm, x3, misc_sem.at[0])
    ga_copy = copy(ga_hbm, ga, misc_sem.at[1])
    wq_copy = copy(wq_hbm, ring.at[2, 7], ring_sem.at[2, 7, 0])
    wo_copy = copy(wo_hbm, wo, misc_sem.at[2])
    gm_copy = copy(gm_hbm, gm, misc_sem.at[3])
    x_copy.start()
    ga_copy.start()
    wq_copy.start()
    fill(0)

    def norm(src, gain, first, count):
        def pair(i, carry):
            wide = jnp.concatenate([src[2 * i], src[2 * i + 1]], axis=0).astype(F32)
            scale = lax.rsqrt(jnp.mean(wide * wide, -1, keepdims=True) + 1e-6)
            rows16[pl.ds(pl.multiple_of(16 * i, 16), 16), :] = (wide * scale * gain[...].astype(F32)[None, :]).astype(BF16)
            return carry
        lax.fori_loop(first, first + count, pair, 0)

    x_copy.wait()
    ga_copy.wait()
    norm(x3, ga, 0, groups // 2)
    wo_copy.start()
    gm_copy.start()
    wq_copy.wait()
    q = jnp.dot(rows16[...], ring[2, 7], preferred_element_type=F32).astype(BF16).astype(F32)
    turned = []
    for s in range(2):
        t = q[:, s * HEAD:(s + 1) * HEAD]
        turned.append(t * turn_ref[0:1, :] + pltpu.roll(t, HEAD // 2, 1) * turn_ref[1:2, :])
    for g in range(groups):
        q_ref[g] = jnp.concatenate([t[8 * g:8 * g + 8] for t in turned], axis=0).astype(BF16).astype(F32)
    wo_copy.wait()
    pl.semaphore_wait(barrier, CHIPS)

    def bufs(*args):
        return [buf.at[args[-1]] for buf in args[:-1]]

    block = half // PARTS
    sum_a = Sum(t3, x3, h3, lambda j, c: (j // 2, c * half + (j % 2) * (half // 2)), half // 2, bufs(r0a, s1a, r1a, 0), sem_a.at[0])
    sum_b, sum_d = [
        Sum(t3, x3, h3, lambda j, c, n=n: (4 + 2 * n + c, j * block), block, bufs(r0b, s1b, r1b, n), sem_b.at[n], 2 * PARTS) for n in range(2)
    ]
    sums_c = [
        Sum(t3, h3, o_ref, lambda j, c, n=n: (j, c * half + n * block), block, bufs(r0c, s1c, r1c, n), sem_c.at[n]) for n in range(PARTS)
    ]

    def attend(g):
        row = lax.broadcasted_iota(jnp.int32, (16, HEAD), 0) % 8
        base = g % 3
        q16 = q_ref[g]
        for i in range(4):
            for j in range(2):
                cache_copy(g, i, j).wait()
        @pl.when(g < groups - 1)
        def _():
            fill(g + 1, KEYS)
        lhs = [
            jnp.concatenate([jnp.where(row == 2 * p + j, q16, 0.0) for j in range(2)], axis=1).astype(BF16)
            for p in range(4)
        ]
        chunk = 512
        for c in range(0, cache, chunk):
            s = None
            for p in range(4):
                part = lax.dot_general(lhs[p], ring[base, p, c:c + chunk, :], NT, preferred_element_type=F32)
                s = part if s is None else s + part
            s_ref[:, c:c + chunk] = s
        s = s_ref[...] * HEAD**-0.5
        e = jnp.exp(s - jnp.max(s, -1, keepdims=True))
        w = (e * (1.0 / jnp.sum(e, -1, keepdims=True))).astype(BF16)
        for i in range(4, 8):
            for j in range(2):
                cache_copy(g, i, j).wait()
        @pl.when(g < groups - 1)
        def _():
            fill(g + 1, VALUES)
        @pl.when(g == groups - 1)
        def _():
            fill_ffn(range(8))
        acc = jnp.zeros((16, HEAD), F32)
        for p in range(4):
            got = jnp.dot(w, ring[base, 4 + p, 0:cache, :], preferred_element_type=F32)
            for j in range(2):
                acc = jnp.where(row == 2 * p + j, got[:, j * HEAD:(j + 1) * HEAD], acc)
        at = pl.ds(pl.multiple_of(8 * g, 8), 8)
        seen[at, 0:HEAD] = acc[0:8]
        seen[at, HEAD:] = acc[8:16]

    def project(first, count):
        rows = seen[8 * first:8 * (first + count), :].astype(BF16)
        for c in range(0, d, 768):
            term = jnp.dot(rows, wo[:, c:c + 768], preferred_element_type=F32)
            for i in range(count):
                t3[first + i, :, c:c + 768] = term[8 * i:8 * i + 8].astype(BF16)

    def body(g, carry):
        attend(g)
        @pl.when(g == 3)
        def _():
            project(0, 4)
            sum_a.send_halves()
        @pl.when(g == 4)
        def _():
            sum_a.send_terms()
        @pl.when(g == 5)
        def _():
            project(4, 2)
            sum_b.send_halves()
            sum_a.finish()
        @pl.when(g == 6)
        def _():
            sum_b.send_terms()
            sum_a.forward()
        @pl.when(g == 7)
        def _():
            sum_b.finish()
        return carry

    lax.fori_loop(0, groups, body, 0)
    project(6, 2)
    sum_d.send_halves()
    fill_ffn(range(8, 16))
    sum_b.forward()
    sum_d.send_terms()
    gm_copy.wait()
    sum_a.settle()
    norm(h3, gm, 0, 2)
    sum_d.finish()
    fill_ffn(range(16, 24))
    sum_b.settle()
    norm(h3, gm, 2, 1)
    sum_d.forward()
    sum_a.sent()
    sum_b.sent()
    sum_d.settle()
    norm(h3, gm, 3, 1)

    sum_d.sent()
    for i in range(3):
        for f in range(6 * i, 6 * i + 6):
            up_copy(f).wait()
        for n in range(3 * i, 3 * i + 3):
            gate = jnp.dot(rows16[...], ring[ffn_slot(2 * n)], preferred_element_type=F32)
            up = jnp.dot(rows16[...], ring[ffn_slot(2 * n + 1)], preferred_element_type=F32)
            hidden[:, n * 256:(n + 1) * 256] = (jax.nn.silu(gate) * up).astype(BF16)
        if i == 0:
            fill_ffn(range(24, 27))

    def down(blocks):
        for k in blocks:
            down_copy(k).wait()
        for k in blocks:
            at = ffn_slot(18 + k // 2)
            term = jnp.dot(hidden[...], ring[at[0], at[1], (k % 2) * ff:(k % 2 + 1) * ff, :], preferred_element_type=F32)
            for i in range(groups):
                t3[i, :, pl.ds(down_column(k), 256)] = term[8 * i:8 * i + 8].astype(BF16)

    c0, c1, c2 = sums_c
    down(range(0, 3))
    c0.send_halves()
    down(range(3, 6))
    down(range(6, 9))
    c1.send_halves()
    c0.send_terms()
    down(range(9, 12))
    down(range(12, 15))
    c2.send_halves()
    c1.send_terms()
    down(range(15, 18))
    c2.send_terms()
    c0.finish()
    c1.finish()
    c0.forward()
    c2.finish()
    c1.forward()
    c2.forward()
    for c in sums_c:
        c.settle()
        c.sent()


def layer(x, k_cache, v_cache, gain_a, wq, wo, gain_m, w_gate, w_up, w_down):
    rows, d = x.shape
    cache = k_cache.shape[1]
    ff = w_gate.shape[1]
    blocks = (CHIPS, rows // CHIPS, d)
    wide = d // 4
    whole, small, large = (1, CHIPS, 8, wide), (2, CHIPS, 8, 2 * wide // PARTS), (PARTS, CHIPS, 8, 2 * wide // PARTS)
    dma = pltpu.SemaphoreType.DMA
    anywhere = pl.BlockSpec(memory_space=pl.ANY)
    vmem = pl.BlockSpec(memory_space=pltpu.VMEM)
    scratch = [
        pltpu.VMEM((3, 8, d, 256), BF16),
        pltpu.VMEM(wo.shape, BF16),
        pltpu.VMEM(blocks, BF16),
        pltpu.VMEM(blocks, BF16),
        pltpu.VMEM(blocks, BF16),
        pltpu.VMEM((rows, d), BF16),
        pltpu.VMEM((rows, ff), BF16),
        pltpu.VMEM((rows // 8, 16, HEAD), F32),
        pltpu.VMEM((rows, 2 * HEAD), F32),
        pltpu.VMEM((16, cache), F32),
        pltpu.VMEM((d,), BF16),
        pltpu.VMEM((d,), BF16),
    ]
    scratch += [pltpu.VMEM(whole, BF16)] * 3 + [pltpu.VMEM(small, BF16)] * 3 + [pltpu.VMEM(large, BF16)] * 3
    scratch += [dma((3, 8, 2)), dma((4,))] + [dma((1, 8, CHIPS))] + [dma((2, 8, CHIPS)), dma((PARTS, 8, CHIPS))]
    out = pl.pallas_call(
        layer_kernel,
        out_shape=jax.ShapeDtypeStruct(blocks, BF16),
        in_specs=[vmem] + [anywhere] * 10,
        out_specs=vmem,
        scratch_shapes=scratch,
        compiler_params=pltpu.CompilerParams(collective_id=0, has_side_effects=True, vmem_limit_bytes=66_200_000),
        name="layer",
    )(
        jnp.asarray(rotation(cache - 1)), x.reshape(blocks), k_cache.reshape(rows, cache, HEAD), v_cache.reshape(rows, cache, HEAD),
        gain_a, wq, wo, gain_m, w_gate, w_up, w_down,
    )
    return out.reshape(x.shape)


def solution(mesh):
    states, cache, columns, rows_of = P("dp", None), P("dp", None, "tp", None), P(None, "tp"), P("tp", None)
    return jax.shard_map(
        layer,
        mesh=mesh,
        in_specs=(states, cache, cache, P(None), columns, rows_of, P(None), columns, columns, rows_of),
        out_specs=states,
        check_vma=False,
    )
```

```python
import functools

import jax
import jax.numpy as jnp
import numpy as np
from jax import lax
from jax.experimental import pallas as pl
from jax.experimental.pallas import tpu as pltpu
from jax.sharding import PartitionSpec as P

HEAD = 128
THETA = 10000
CHIPS = 8
PARTS = 3
KEYS, VALUES = range(4), range(4, 8)
MESH = pl.DeviceIdType.MESH
F32, BF16 = jnp.float32, jnp.bfloat16
NT = (((1,), (1,)), ((), ()))


def rotation(place):
    half = HEAD // 2
    step = np.float32(THETA) ** (-np.arange(half, dtype=np.float32) / np.float32(half))
    angle = (np.float32(place) * step).astype(np.float64)
    cos, sin = np.cos(angle), np.sin(angle)
    return np.stack([np.concatenate([cos, cos]), np.concatenate([-sin, sin])]).astype(np.float32)


class Sum:
    def __init__(self, t, residual, out, place, wide, bufs, sems, owners=CHIPS):
        self.t, self.residual, self.out, self.place, self.wide, self.owners = t, residual, out, place, wide, owners
        self.r0, self.s1, self.r1 = bufs
        self.sems = sems
        me = lax.axis_index("tp")
        self.core, self.chip = me % 2, me // 2
        self.partner = me + 1 - 2 * self.core

    def to(self, o):
        return (self.chip + o) % CHIPS

    def frm(self, o):
        return (self.chip + CHIPS - o) % CHIPS

    def at(self, j, core):
        block, column = self.place(j, core)
        return block, slice(None), pl.ds(pl.multiple_of(column, 128), self.wide)

    def owned(self, j, act):
        if self.owners == CHIPS:
            act()
        else:
            pl.when(j < self.owners)(act)

    def remote(self, src, dst, kind, o, device):
        return pltpu.make_async_remote_copy(
            src_ref=src, dst_ref=dst, send_sem=self.sems.at[kind, o], recv_sem=self.sems.at[kind + 1, o],
            device_id={"tp": device}, device_id_type=MESH,
        )

    def halves(self, o):
        return self.remote(self.t.at[self.at(self.to(o), 1 - self.core)], self.r0.at[o], 0, o, self.partner)

    def terms(self, o):
        return self.remote(self.s1.at[o], self.r1.at[o], 2, o, self.to(o) * 2 + self.core)

    def shares(self, o, chip):
        done = self.out.at[self.at(chip, self.core)]
        return self.remote(done, done, 4, o, self.to(o) * 2 + self.core)

    def over(self, o):
        piece = self.out.at[self.at(self.frm(o), self.core)]
        return self.remote(piece, piece, 6, o, self.partner)

    def send_halves(self):
        for o in [*range(1, CHIPS), 0]:
            self.owned(self.to(o), lambda o=o: self.halves(o).start())

    def send_terms(self):
        def send(o):
            self.halves(o).wait_recv()
            self.s1[o] = (self.t[self.at(self.to(o), self.core)].astype(F32) + self.r0[o].astype(F32)).astype(BF16)
            self.terms(o).start()

        for o in range(1, CHIPS):
            self.owned(self.to(o), lambda o=o: send(o))

    def finish(self):
        def act():
            self.halves(0).wait_recv()
            mine = self.at(self.chip, self.core)
            total = self.t[mine].astype(F32) + self.r0[0].astype(F32)
            for o in range(1, CHIPS):
                self.terms(o).wait_recv()
                total = total + self.r1[o].astype(F32)
            self.out[mine] = (self.residual[mine].astype(F32) + total).astype(BF16)
            for o in range(1, CHIPS):
                self.shares(o, self.chip).start()
            self.over(0).start()

        self.owned(self.chip, act)

    def forward(self):
        def act(o):
            self.shares(o, self.frm(o)).wait_recv()
            self.over(o).start()

        for o in range(1, CHIPS):
            self.owned(self.frm(o), lambda o=o: act(o))

    def settle(self):
        for o in range(CHIPS):
            self.owned(self.frm(o), lambda o=o: self.over(o).wait_recv())

    def sent(self):
        for o in range(CHIPS):
            self.owned(self.to(o), lambda o=o: self.halves(o).wait_send())
            self.owned(self.frm(o), lambda o=o: self.over(o).wait_send())
            if o:
                self.owned(self.to(o), lambda o=o: self.terms(o).wait_send())
                self.owned(self.chip, lambda o=o: self.shares(o, self.chip).wait_send())


def layer_kernel(
    turn_ref, x_hbm, k_hbm, v_hbm, ga_hbm, wq_hbm, wo_hbm, gm_hbm, wg_hbm, wu_hbm, wd_hbm, o_ref,
    ring, wo, x3, h3, t3, rows16, hidden, q_ref, seen, s_ref, ga, gm,
    r0a, s1a, r1a, r0b, s1b, r1b, r0c, s1c, r1c,
    ring_sem, misc_sem, sem_a, sem_b, sem_c,
):
    d = x3.shape[2]
    half = d // 2
    cache = k_hbm.shape[1]
    ff = wg_hbm.shape[1]
    groups = x3.shape[0]
    me = lax.axis_index("tp")
    core, chip = me % 2, me // 2
    partner = me + 1 - 2 * core

    barrier = pltpu.get_barrier_semaphore()
    pl.semaphore_signal(barrier, inc=1, device_id={"tp": partner}, device_id_type=MESH)
    for o in range(1, CHIPS):
        pl.semaphore_signal(barrier, inc=1, device_id={"tp": (chip + o) % CHIPS * 2 + core}, device_id_type=MESH)

    def copy(src, dst, sem):
        return pltpu.make_async_copy(src, dst, sem)

    def cache_copy(g, i, j):
        src = k_hbm if i < 4 else v_hbm
        b = g * 8 + 2 * (i % 4) + j
        return copy(src.at[b], ring.at[g % 3, i, 0:cache, j * HEAD:(j + 1) * HEAD], ring_sem.at[g % 3, i, j])

    def fill(g, slots=range(8)):
        for i in slots:
            for j in range(2):
                cache_copy(g, i, j).start()

    def ffn_slot(f):
        return (groups + f // 8) % 3, f % 8

    def up_copy(f):
        src = (wg_hbm, wu_hbm)[f % 2]
        at = ffn_slot(f)
        return copy(src.at[:, (f // 2) * 256:(f // 2 + 1) * 256], ring.at[at], ring_sem.at[at[0], at[1], 0])

    def down_column(k):
        side = core if k % 6 >= 3 else 1 - core
        return pl.multiple_of(side * half + k // 6 * (half // PARTS) + k % 3 * 256, 128)

    def down_copy(k):
        at = ffn_slot(18 + k // 2)
        return copy(wd_hbm.at[:, pl.ds(down_column(k), 256)], ring.at[at[0], at[1], (k % 2) * ff:(k % 2 + 1) * ff], ring_sem.at[at[0], at[1], k % 2])

    def fill_ffn(slots):
        for f in slots:
            if f < 18:
                up_copy(f).start()
            else:
                down_copy(2 * (f - 18)).start()
                down_copy(2 * (f - 18) + 1).start()

    x_copy = copy(x_hbm, x3, misc_sem.at[0])
    ga_copy = copy(ga_hbm, ga, misc_sem.at[1])
    wq_copy = copy(wq_hbm, ring.at[2, 7], ring_sem.at[2, 7, 0])
    wo_copy = copy(wo_hbm, wo, misc_sem.at[2])
    gm_copy = copy(gm_hbm, gm, misc_sem.at[3])
    x_copy.start()
    ga_copy.start()
    wq_copy.start()
    fill(0)

    def norm(src, gain, first, count):
        def pair(i, carry):
            wide = jnp.concatenate([src[2 * i], src[2 * i + 1]], axis=0).astype(F32)
            scale = lax.rsqrt(jnp.mean(wide * wide, -1, keepdims=True) + 1e-6)
            rows16[pl.ds(pl.multiple_of(16 * i, 16), 16), :] = (wide * scale * gain[...].astype(F32)[None, :]).astype(BF16)
            return carry
        lax.fori_loop(first, first + count, pair, 0)

    x_copy.wait()
    ga_copy.wait()
    norm(x3, ga, 0, groups // 2)
    wo_copy.start()
    gm_copy.start()
    wq_copy.wait()
    q = jnp.dot(rows16[...], ring[2, 7], preferred_element_type=F32).astype(BF16).astype(F32)
    turned = []
    for s in range(2):
        t = q[:, s * HEAD:(s + 1) * HEAD]
        turned.append(t * turn_ref[0:1, :] + pltpu.roll(t, HEAD // 2, 1) * turn_ref[1:2, :])
    for g in range(groups):
        q_ref[g] = jnp.concatenate([t[8 * g:8 * g + 8] for t in turned], axis=0).astype(BF16).astype(F32)
    wo_copy.wait()
    pl.semaphore_wait(barrier, CHIPS)

    def bufs(*args):
        return [buf.at[args[-1]] for buf in args[:-1]]

    block = half // PARTS
    sum_a, sum_b = [
        Sum(t3, x3, h3, lambda j, c, n=n: (4 * n + j // 2, c * half + (j % 2) * (half // 2)), half // 2, share, sems.at[0])
        for n, (share, sems) in enumerate([(bufs(r0a, s1a, r1a, 0), sem_a), (bufs(r0b, s1b, r1b, 0), sem_b)])
    ]
    sums_c = [
        Sum(t3, h3, o_ref, lambda j, c, n=n: (j, c * half + n * block), block, bufs(r0c, s1c, r1c, n), sem_c.at[n]) for n in range(PARTS)
    ]

    def attend(g):
        row = lax.broadcasted_iota(jnp.int32, (16, HEAD), 0) % 8
        base = g % 3
        q16 = q_ref[g]
        for i in range(4):
            for j in range(2):
                cache_copy(g, i, j).wait()
        @pl.when(g < groups - 1)
        def _():
            fill(g + 1, KEYS)
        lhs = [
            jnp.concatenate([jnp.where(row == 2 * p + j, q16, 0.0) for j in range(2)], axis=1).astype(BF16)
            for p in range(4)
        ]
        chunk = 512
        for c in range(0, cache, chunk):
            s = None
            for p in range(4):
                part = lax.dot_general(lhs[p], ring[base, p, c:c + chunk, :], NT, preferred_element_type=F32)
                s = part if s is None else s + part
            s_ref[:, c:c + chunk] = s
        s = s_ref[...] * HEAD**-0.5
        e = jnp.exp(s - jnp.max(s, -1, keepdims=True))
        w = (e * (1.0 / jnp.sum(e, -1, keepdims=True))).astype(BF16)
        for i in range(4, 8):
            for j in range(2):
                cache_copy(g, i, j).wait()
        @pl.when(g < groups - 1)
        def _():
            fill(g + 1, VALUES)
        @pl.when(g == groups - 1)
        def _():
            fill_ffn(range(8))
        acc = jnp.zeros((16, HEAD), F32)
        for p in range(4):
            got = jnp.dot(w, ring[base, 4 + p, 0:cache, :], preferred_element_type=F32)
            for j in range(2):
                acc = jnp.where(row == 2 * p + j, got[:, j * HEAD:(j + 1) * HEAD], acc)
        at = pl.ds(pl.multiple_of(8 * g, 8), 8)
        seen[at, 0:HEAD] = acc[0:8]
        seen[at, HEAD:] = acc[8:16]

    def project(first, count):
        rows = seen[8 * first:8 * (first + count), :].astype(BF16)
        for c in range(0, d, 768):
            term = jnp.dot(rows, wo[:, c:c + 768], preferred_element_type=F32)
            for i in range(count):
                t3[first + i, :, c:c + 768] = term[8 * i:8 * i + 8].astype(BF16)

    def body(g, carry):
        attend(g)
        @pl.when(g == 3)
        def _():
            project(0, 4)
            sum_a.send_halves()
        @pl.when(g == 4)
        def _():
            sum_a.send_terms()
        @pl.when(g == 5)
        def _():
            sum_a.finish()
        @pl.when(g == 6)
        def _():
            sum_a.forward()
        return carry

    lax.fori_loop(0, groups, body, 0)
    project(4, 4)
    sum_b.send_halves()
    fill_ffn(range(8, 16))
    sum_b.send_terms()
    gm_copy.wait()
    sum_a.settle()
    norm(h3, gm, 0, 2)
    sum_b.finish()
    fill_ffn(range(16, 24))
    sum_a.sent()
    sum_b.forward()
    sum_b.settle()
    norm(h3, gm, 2, 2)
    sum_b.sent()
    for i in range(3):
        for f in range(6 * i, 6 * i + 6):
            up_copy(f).wait()
        for n in range(3 * i, 3 * i + 3):
            gate = jnp.dot(rows16[...], ring[ffn_slot(2 * n)], preferred_element_type=F32)
            up = jnp.dot(rows16[...], ring[ffn_slot(2 * n + 1)], preferred_element_type=F32)
            hidden[:, n * 256:(n + 1) * 256] = (jax.nn.silu(gate) * up).astype(BF16)
        if i == 0:
            fill_ffn(range(24, 27))

    def down(blocks):
        for k in blocks:
            down_copy(k).wait()
        for k in blocks:
            at = ffn_slot(18 + k // 2)
            term = jnp.dot(hidden[...], ring[at[0], at[1], (k % 2) * ff:(k % 2 + 1) * ff, :], preferred_element_type=F32)
            for i in range(groups):
                t3[i, :, pl.ds(down_column(k), 256)] = term[8 * i:8 * i + 8].astype(BF16)

    c0, c1, c2 = sums_c
    down(range(0, 3))
    c0.send_halves()
    down(range(3, 6))
    down(range(6, 9))
    c1.send_halves()
    c0.send_terms()
    down(range(9, 12))
    down(range(12, 15))
    c2.send_halves()
    c1.send_terms()
    down(range(15, 18))
    c2.send_terms()
    c0.finish()
    c1.finish()
    c0.forward()
    c2.finish()
    c1.forward()
    c2.forward()
    for c in sums_c:
        c.settle()
        c.sent()


def layer(x, k_cache, v_cache, gain_a, wq, wo, gain_m, w_gate, w_up, w_down):
    rows, d = x.shape
    cache = k_cache.shape[1]
    ff = w_gate.shape[1]
    blocks = (CHIPS, rows // CHIPS, d)
    wide = d // 4
    whole, large = (1, CHIPS, 8, wide), (PARTS, CHIPS, 8, 2 * wide // PARTS)
    dma = pltpu.SemaphoreType.DMA
    anywhere = pl.BlockSpec(memory_space=pl.ANY)
    vmem = pl.BlockSpec(memory_space=pltpu.VMEM)
    scratch = [
        pltpu.VMEM((3, 8, d, 256), BF16),
        pltpu.VMEM(wo.shape, BF16),
        pltpu.VMEM(blocks, BF16),
        pltpu.VMEM(blocks, BF16),
        pltpu.VMEM(blocks, BF16),
        pltpu.VMEM((rows, d), BF16),
        pltpu.VMEM((rows, ff), BF16),
        pltpu.VMEM((rows // 8, 16, HEAD), F32),
        pltpu.VMEM((rows, 2 * HEAD), F32),
        pltpu.VMEM((16, cache), F32),
        pltpu.VMEM((d,), BF16),
        pltpu.VMEM((d,), BF16),
    ]
    scratch += [pltpu.VMEM(whole, BF16)] * 6 + [pltpu.VMEM(large, BF16)] * 3
    scratch += [dma((3, 8, 2)), dma((4,))] + [dma((1, 8, CHIPS))] * 2 + [dma((PARTS, 8, CHIPS))]
    out = pl.pallas_call(
        layer_kernel,
        out_shape=jax.ShapeDtypeStruct(blocks, BF16),
        in_specs=[vmem] + [anywhere] * 10,
        out_specs=vmem,
        scratch_shapes=scratch,
        compiler_params=pltpu.CompilerParams(collective_id=0, has_side_effects=True, vmem_limit_bytes=66_200_000),
        name="layer",
    )(
        jnp.asarray(rotation(cache - 1)), x.reshape(blocks), k_cache.reshape(rows, cache, HEAD), v_cache.reshape(rows, cache, HEAD),
        gain_a, wq, wo, gain_m, w_gate, w_up, w_down,
    )
    return out.reshape(x.shape)


def solution(mesh):
    states, cache, columns, rows_of = P("dp", None), P("dp", None, "tp", None), P(None, "tp"), P("tp", None)
    return jax.shard_map(
        layer,
        mesh=mesh,
        in_specs=(states, cache, cache, P(None), columns, rows_of, P(None), columns, columns, rows_of),
        out_specs=states,
        check_vma=False,
    )
```
